256 devices in a mesh: dp: 8 (over x, core), table: 32 (over y, z).
Axes of the slice: x: 4, y: 4, z: 8, core: 2. Of those that a mesh axis runs over, the one named last changes fastest.
Arguments:
- out_grad: bfloat16 [262144, 1024], P(('dp', 'table')), may hold values from -0.125 to 0.125
- pair_cells: int32 [262144, 8, 32], P(('dp', 'table')), may hold values from 0 to 4095
- weight_codes: int32 [262144, 8, 32], P(('dp', 'table')), may hold values from -127 to 127
- head_scale: float32 [8], replicated, may hold values from 0.5 to 2
- touch_slots: int32 [32, 32, 1], replicated, may hold values from 0 to 7
Outputs:
- grad_rows: bfloat16 [32768, 1024], P('table', 'dp')
The draws below stay inside these ranges and needn't reach their ends.
All inputs are finite; a program needn't handle non-finite values.
Results may differ from the reference program's by a relative error of at most 0.0098.
Values may be sent and summed in bfloat16 or wider, within the bound.
A program may use at most 128 MiB of HBM per device.

```python
import math
import jax
import jax.numpy as jnp
from jax import lax

V = 1024
HEADS = 8
TOPK = 32
ROWS = 128
TOUCH = 32
OWN = 8
TOK_DEV = 1024
CAP = 1
TOKENS = 262144
N_DP = 8
N_TABLE = 32


def set_ends(result, key, low, top_value):
    spot = [jax.random.randint(jax.random.fold_in(key, axis), (), 0, length) for axis, length in enumerate(result.shape)]
    longest = result.shape.index(max(result.shape))
    beside = spot[:longest] + [(spot[longest] + 1) % result.shape[longest]] + spot[longest + 1:]
    return result.at[tuple(spot)].set(low).at[tuple(beside)].set(top_value)


def level_of(own_key, shape, shards, least, largest):
    def one(axis_at, shards_of):
        draws = jax.random.uniform(jax.random.fold_in(jax.random.fold_in(own_key, 6), axis_at), (shards_of,), jnp.float32, least / len(shards), largest / len(shards))
        return jnp.repeat(jnp.exp(draws), shape[axis_at] // shards_of).reshape((-1,) + (1,) * (len(shape) - axis_at - 1))

    loudness = one(*shards[0])
    for cut in shards[1:]:
        loudness = loudness * one(*cut)
    return loudness


def gaussian(own_key, extent, spread, reach, shards=(), held_as=jnp.bfloat16):
    drawn = jax.random.normal(own_key, extent, jnp.float32) * spread
    if len(shards) > 0:
        drawn = level_of(own_key, extent, shards, -0.22, 0.18) * drawn
    return jnp.clip(drawn, min=-reach, max=reach).astype(held_as)


def setup_inputs(seed: int = 0) -> dict:
    keys = jax.random.split(jax.random.key(seed), 6)
    out_grad = gaussian(keys[0], (TOKENS, V), ((ROWS * OWN) ** 0.5 / (N_DP * TOK_DEV * HEADS * TOPK) ** 0.5), 0.125, ((0, 256),))
    pair_cells = set_ends(jax.random.randint(keys[1], (TOKENS, HEADS, TOPK), 0, TOUCH * ROWS), jax.random.fold_in(keys[1], 1), 0, (TOUCH * ROWS) - 1).astype(jnp.int32)
    weight_codes = set_ends(jax.random.randint(keys[2], (TOKENS, HEADS, TOPK), -127, 128), jax.random.fold_in(keys[2], 1), -127, 127).astype(jnp.int32)
    head_scale = jnp.clip(jnp.exp(jax.random.uniform(keys[3], (HEADS,), jnp.float32, math.log(0.5), math.log(2.0))), 0.5, 2.0)
    touch_slots = set_ends(jax.random.randint(keys[4], (N_TABLE, N_TABLE, CAP), 0, OWN), jax.random.fold_in(keys[4], 1), 0, OWN - 1).astype(jnp.int32)
    return {"out_grad": out_grad, "pair_cells": pair_cells, "weight_codes": weight_codes, "head_scale": head_scale, "touch_slots": touch_slots}


def reference(out_grad, pair_cells, weight_codes, head_scale, touch_slots):
    devices = N_DP * N_TABLE
    weight = weight_codes.astype(jnp.float32) * head_scale[None, :, None].astype(jnp.float32) / 128.0
    cells = pair_cells.reshape(devices, TOK_DEV, HEADS * TOPK)
    weights = weight.reshape(devices, TOK_DEV, HEADS * TOPK)
    grads = out_grad.reshape(devices, TOK_DEV, V).astype(jnp.float32)
    tok_iota = jnp.arange(TOK_DEV, dtype=jnp.int32)
    cap = TOUCH // N_TABLE

    def one(total, index):
        group = index % N_TABLE
        coef = jnp.zeros((TOUCH * ROWS, TOK_DEV), jnp.float32)
        coef = coef.at[cells[index], tok_iota[:, None]].add(weights[index])
        coef = lax.optimization_barrier(coef.astype(jnp.bfloat16)).astype(jnp.float32)
        partial_value = jnp.dot(coef, grads[index], precision=lax.Precision.HIGHEST)
        owners = jnp.arange(N_TABLE, dtype=jnp.int32)[:, None] * OWN
        target = (owners + touch_slots[group].astype(jnp.int32)).reshape(N_TABLE * cap)
        total = total.at[target].add(partial_value.reshape(TOUCH, ROWS, V))
        return total, None

    start = jnp.zeros((N_TABLE * OWN, ROWS, V), jnp.float32)
    total, _ = lax.scan(one, start, jnp.arange(devices, dtype=jnp.int32))
    return total.reshape(N_TABLE * OWN * ROWS, V).astype(jnp.bfloat16)
```

```python
import functools

import jax
import jax.numpy as jnp
from jax import lax
from jax.experimental import pallas as pl
from jax.experimental.pallas import tpu as pltpu
from jax.sharding import PartitionSpec as P

ROWS = 128
TOUCH = 32
OWN = 8
NX = 4
NY = 4
NZ = 8
MESH = pl.DeviceIdType.MESH
BF = jnp.bfloat16
F32 = jnp.float32


def coef_kernel(block, unroll, stride, scale_ref, cells_ref, codes_ref, grad_ref, coef_ref, gt_ref,
                row_ref, tile_ref, weight_ref, table_ref):
    pairs = cells_ref.shape[0]
    heads = scale_ref.shape[0]
    per = pairs // heads
    cells = cells_ref[...]
    row_ref[...] = (cells % ROWS).astype(F32).T.astype(BF)
    tile_ref[...] = (cells // ROWS).astype(F32).T.astype(BF)
    weight = jnp.concatenate(
        [
            codes_ref[h * per : (h + 1) * per, :].astype(F32) * (scale_ref[h] / 128.0)
            for h in range(heads)
        ],
        axis=0,
    )
    weight_ref[...] = weight.T.astype(BF)
    for b in range(grad_ref.shape[1] // ROWS):
        gt_ref[b * ROWS : (b + 1) * ROWS, :] = grad_ref[:, b * ROWS : (b + 1) * ROWS].T
    row_iota = lax.broadcasted_iota(jnp.int32, (ROWS, pairs), 0).astype(F32).astype(BF)
    tile_iota = lax.broadcasted_iota(jnp.int32, (TOUCH, pairs), 0).astype(F32).astype(BF)
    one = jnp.ones((), BF)
    zero = jnp.zeros((), BF)

    def step(g, carry):
        base = pl.multiple_of(g * unroll, unroll)
        row = row_ref[pl.ds(base, unroll), :]
        tile = tile_ref[pl.ds(base, unroll), :]
        weights = weight_ref[pl.ds(base, unroll), :]
        for u in range(unroll):
            row_hot = jnp.where(
                jnp.broadcast_to(row[u : u + 1, :], (ROWS, pairs)) == row_iota, one, zero
            ).astype(jnp.float8_e4m3fn)
            tile_hot = jnp.where(
                jnp.broadcast_to(tile[u : u + 1, :], (TOUCH, pairs)) == tile_iota,
                jnp.broadcast_to(weights[u : u + 1, :], (TOUCH, pairs)),
                zero,
            )
            table_ref[pl.ds(base + u, TOUCH, stride=stride), :] = lax.dot_general(
                tile_hot, row_hot, (((1,), (1,)), ((), ())), preferred_element_type=F32
            )
        return carry

    lax.fori_loop(0, block // unroll, step, 0)

    def flush(j, carry):
        coef_ref[j] = table_ref[pl.ds(pl.multiple_of(j * stride, 8), block), :].astype(BF)
        return carry

    lax.fori_loop(0, TOUCH, flush, 0, unroll=8)


def coef_tables(cells, codes, head_scale, out_grad, block=128, unroll=64):
    pairs, tokens = cells.shape
    width = out_grad.shape[1]
    stride = block + 8
    return pl.pallas_call(
        functools.partial(coef_kernel, block, unroll, stride),
        grid=(tokens // block,),
        in_specs=[
            pl.BlockSpec(memory_space=pltpu.SMEM),
            pl.BlockSpec((pairs, block), lambda i: (0, i)),
            pl.BlockSpec((pairs, block), lambda i: (0, i)),
            pl.BlockSpec((block, width), lambda i: (i, 0)),
        ],
        out_specs=[
            pl.BlockSpec((TOUCH, block, ROWS), lambda i: (0, i, 0)),
            pl.BlockSpec((width, block), lambda i: (0, i)),
        ],
        out_shape=[
            jax.ShapeDtypeStruct((TOUCH, tokens, ROWS), BF),
            jax.ShapeDtypeStruct((width, tokens), BF),
        ],
        scratch_shapes=[pltpu.VMEM((block, pairs), BF)] * 3
        + [pltpu.VMEM((TOUCH * stride, ROWS), F32)],
        compiler_params=pltpu.CompilerParams(vmem_limit_bytes=48 << 20),
        name="coef_tables",
    )(head_scale, cells, codes, out_grad)


def exchange_kernel(slots_ref, coef_ref, gt_ref, out_ref,
                    grads, coefs, own, pair_out, pair_in,
                    opp_out, opp_in, near_out, near_in, keep, fin0, tiles, got, acc,
                    grad_sem, coef_sem, pair_send, pair_recv,
                    opp_send, opp_recv, near_send, near_recv, tile_send, tile_recv):
    dp = lax.axis_index("dp")
    table = lax.axis_index("table")
    x, c = lax.div(dp, 2), lax.rem(dp, 2)
    y, z = lax.div(table, NZ), lax.rem(table, NZ)
    half = NY // 2
    partner = (x * 2 + 1 - c, table)
    ahead = (lax.rem(x + 1, NX) * 2 + c, table)
    behind = (lax.rem(x + NX - 1, NX) * 2 + c, table)
    sides = (ahead, behind)

    def dz_of(s):
        odd = lax.rem(s, 2)
        return lax.rem(NZ // 2 + (1 - 2 * odd) * lax.div(s + 1, 2), NZ)

    def tile_of(s, i):
        return lax.rem(y + i, NY) * NZ + lax.rem(z + dz_of(s), NZ)

    def source_of(s, i):
        return lax.rem(y + NY - i, NY) * NZ + lax.rem(z + NZ - dz_of(s), NZ)

    barrier = pltpu.get_barrier_semaphore()

    def greet(k, carry):
        pl.semaphore_signal(
            barrier, inc=1, device_id=(dp, lax.rem(table + k, NY * NZ)), device_id_type=MESH
        )
        return carry

    for peer in (partner, ahead, behind):
        pl.semaphore_signal(barrier, inc=1, device_id=peer, device_id_type=MESH)
    lax.fori_loop(1, NY * NZ, greet, 0)

    def grad_copy(k):
        r = k % NX
        core = (1 - c) if k < NX else c
        block = lax.rem(x + r, NX) * 2 + core
        return pltpu.make_async_copy(
            gt_ref.at[pl.ds(pl.multiple_of(block * ROWS, ROWS), ROWS), :],
            grads.at[pl.ds(k * ROWS, ROWS), :],
            grad_sem.at[k],
        )

    def coef_copy(s, i):
        slot = lax.rem(s, 2)
        return pltpu.make_async_copy(
            coef_ref.at[tile_of(s, i)],
            coefs.at[slot, :, pl.ds(i * ROWS, ROWS)],
            coef_sem.at[slot, i],
        )

    def pair_copy(q):
        return pltpu.make_async_remote_copy(
            src_ref=pair_out.at[q], dst_ref=pair_in.at[q],
            send_sem=pair_send.at[q], recv_sem=pair_recv.at[q],
            device_id=partner, device_id_type=MESH,
        )

    def opp_copy(q, side):
        return pltpu.make_async_remote_copy(
            src_ref=opp_out.at[q, side], dst_ref=opp_in.at[q, side],
            send_sem=opp_send.at[q, side], recv_sem=opp_recv.at[q, side],
            device_id=sides[side], device_id_type=MESH,
        )

    def near_copy(q, side, part):
        return pltpu.make_async_remote_copy(
            src_ref=near_out.at[q, side, part], dst_ref=near_in.at[q, side, part],
            send_sem=near_send.at[q, side, part], recv_sem=near_recv.at[q, side, part],
            device_id=sides[side], device_id_type=MESH,
        )

    def tile_copy(s, i):
        return pltpu.make_async_remote_copy(
            src_ref=tiles.at[s, i], dst_ref=got.at[s, i],
            send_sem=tile_send.at[s, i], recv_sem=tile_recv.at[s, i],
            device_id=(dp, tile_of(s, i)), device_id_type=MESH,
        )

    for i in range(NY):
        coef_copy(0, i).start()
    for k in range(2 * NX):
        grad_copy(k).start()
    for k in range(2 * NX):
        grad_copy(k).wait()
    acc[...] = jnp.zeros_like(acc)

    def product(s, which):
        return jnp.dot(
            grads[which * NX * ROWS : (which + 1) * NX * ROWS, :], coefs[lax.rem(s, 2)],
            preferred_element_type=F32,
        )

    def stage1(s):
        @pl.when(s + 1 < NZ)
        def _():
            for i in range(NY):
                coef_copy(s + 1, i).start()

        for i in range(NY):
            coef_copy(s, i).wait()
        theirs = product(s, 0).astype(BF)
        for r in range(NX):
            for i in range(NY):
                pair_out[s, r, i] = theirs[r * ROWS : (r + 1) * ROWS, i * ROWS : (i + 1) * ROWS]

        @pl.when(s == 0)
        def _():
            pl.semaphore_wait(barrier, NY * NZ + 2)

        pair_copy(s).start()
        mine = product(s, 1)
        slot = lax.rem(s, 2)
        for r in range(NX):
            for i in range(NY):
                own[slot, r, i] = mine[r * ROWS : (r + 1) * ROWS, i * ROWS : (i + 1) * ROWS]

    def stage2(q):
        pair_copy(q).wait_recv()
        slot = lax.rem(q, 2)
        four = lax.rem(q, 4)

        def summed(r, lo):
            return own[slot, r, lo : lo + half] + pair_in[q, r, lo : lo + half].astype(F32)

        for side in range(2):
            opp_out[q, side] = summed(2, side * half).astype(BF)
            opp_copy(q, side).start()
        for side in range(2):
            r = 1 if side == 0 else NX - 1
            near_out[q, side, 0] = summed(r, (1 - side) * half).astype(BF)
            near_copy(q, side, 0).start()
        for side in range(2):
            r = 1 if side == 0 else NX - 1
            keep[slot, side] = summed(r, side * half)
        for part in range(2):
            fin0[four, part * half : (part + 1) * half] = summed(0, part * half)

    def stage3(q):
        slot = lax.rem(q, 2)
        for side in range(2):
            opp_copy(q, side).wait_recv()
            near_out[q, side, 1] = (keep[slot, side] + opp_in[q, side].astype(F32)).astype(BF)
            near_copy(q, side, 1).start()

    def stage4(q):
        four = lax.rem(q, 4)
        for side in range(2):
            for part in range(2):
                near_copy(q, side, part).wait_recv()
        for h in range(2):
            lo = h * half
            total = fin0[four, lo : lo + half]
            for side in range(2):
                part = 1 if side == h else 0
                total = total + near_in[q, side, part].astype(F32)
            tiles[q, lo : lo + half] = total.astype(BF)
        for i in range(NY):
            if i == 0:
                @pl.when(q < NZ - 1)
                def _():
                    tile_copy(q, 0).start()
            else:
                tile_copy(q, i).start()

    def step(s, carry):
        pl.when(s < NZ)(lambda: stage1(s))
        pl.when((s >= 1) & (s < NZ + 1))(lambda: stage2(s - 1))
        pl.when((s >= 2) & (s < NZ + 2))(lambda: stage3(s - 2))
        pl.when(s >= 3)(lambda: stage4(s - 3))
        return carry

    lax.fori_loop(0, NZ + 3, step, 0)

    def gather(s, carry):
        for i in range(NY):
            if i == 0:
                @pl.when(s < NZ - 1)
                def _():
                    tile_copy(s, 0).wait_recv()

                @pl.when(s == NZ - 1)
                def _():
                    got[s, 0] = tiles[s, 0]
            else:
                tile_copy(s, i).wait_recv()
        slots = [slots_ref[source_of(s, i), table] for i in range(NY)]
        parts = [got[s, i].astype(F32) for i in range(NY)]
        for k in range(OWN):
            total = acc[k]
            for i in range(NY):
                total = total + jnp.where(slots[i] == k, parts[i], 0.0)
            acc[k] = total
        return carry

    lax.fori_loop(0, NZ, gather, 0)
    for k in range(OWN):
        out_ref[k * ROWS : (k + 1) * ROWS, :] = acc[k].T.astype(BF)

    def drain(q, carry):
        pair_copy(q).wait_send()
        for side in range(2):
            opp_copy(q, side).wait_send()
            for part in range(2):
                near_copy(q, side, part).wait_send()
        for i in range(NY):
            if i == 0:
                @pl.when(q < NZ - 1)
                def _():
                    tile_copy(q, 0).wait_send()
            else:
                tile_copy(q, i).wait_send()
        return carry

    lax.fori_loop(0, NZ, drain, 0)


def exchange(slots, coef, grads):
    tokens = coef.shape[1]
    half = NY // 2
    tile = (ROWS, ROWS)
    dma = pltpu.SemaphoreType.DMA
    return pl.pallas_call(
        exchange_kernel,
        in_specs=[
            pl.BlockSpec(memory_space=pltpu.SMEM),
            pl.BlockSpec(memory_space=pl.ANY),
            pl.BlockSpec(memory_space=pl.ANY),
        ],
        out_specs=pl.BlockSpec(memory_space=pltpu.VMEM),
        out_shape=jax.ShapeDtypeStruct((OWN * ROWS, ROWS), BF),
        scratch_shapes=[
            pltpu.VMEM((2 * NX * ROWS, tokens), BF),
            pltpu.VMEM((2, tokens, NY * ROWS), BF),
            pltpu.VMEM((2, NX, NY) + tile, F32),
            pltpu.VMEM((NZ, NX, NY) + tile, BF),
            pltpu.VMEM((NZ, NX, NY) + tile, BF),
            pltpu.VMEM((NZ, 2, half) + tile, BF),
            pltpu.VMEM((NZ, 2, half) + tile, BF),
            pltpu.VMEM((NZ, 2, 2, half) + tile, BF),
            pltpu.VMEM((NZ, 2, 2, half) + tile, BF),
            pltpu.VMEM((2, 2, half) + tile, F32),
            pltpu.VMEM((4, NY) + tile, F32),
            pltpu.VMEM((NZ, NY) + tile, BF),
            pltpu.VMEM((NZ, NY) + tile, BF),
            pltpu.VMEM((OWN,) + tile, F32),
            dma((2 * NX,)),
            dma((2, NY)),
            dma((NZ,)),
            dma((NZ,)),
            dma((NZ, 2)),
            dma((NZ, 2)),
            dma((NZ, 2, 2)),
            dma((NZ, 2, 2)),
            dma((NZ, NY)),
            dma((NZ, NY)),
        ],
        compiler_params=pltpu.CompilerParams(
            collective_id=0, has_side_effects=True, vmem_limit_bytes=60 << 20
        ),
        name="exchange",
    )(slots, coef, grads)


def body(out_grad, pair_cells, weight_codes, head_scale, touch_slots):
    tokens = out_grad.shape[0]
    pairs = pair_cells.shape[1] * pair_cells.shape[2]
    cells = pair_cells.transpose(1, 2, 0).reshape(pairs, tokens)
    codes = weight_codes.transpose(1, 2, 0).reshape(pairs, tokens)
    coef, grads = coef_tables(cells, codes, head_scale, out_grad)
    return exchange(touch_slots.reshape(touch_slots.shape[0], -1), coef, grads)


def solution(mesh):
    return jax.shard_map(
        body,
        mesh=mesh,
        in_specs=(
            P(("dp", "table"), None),
            P(("dp", "table"), None, None),
            P(("dp", "table"), None, None),
            P(),
            P(),
        ),
        out_specs=P("table", "dp"),
        check_vma=False,
    )
```

```python
import functools

import jax
import jax.numpy as jnp
from jax import lax
from jax.experimental import pallas as pl
from jax.experimental.pallas import tpu as pltpu
from jax.sharding import PartitionSpec as P

ROWS = 128
TOUCH = 32
OWN = 8
NX = 4
NY = 4
NZ = 8
PARTS = 2
PART = ROWS // PARTS
PAIRED = TOUCH // PARTS
BLOCK = 128
STRIDE = BLOCK + 8
STEPS = PARTS * NZ
MESH = pl.DeviceIdType.MESH
BF = jnp.bfloat16
F32 = jnp.float32


def kernel(scale_ref, slots_ref, cells_hbm, codes_hbm, grad_hbm, out_ref,
           cells, codes, grad, row_of, tile_of_pair, weight_of, table, coefs, grads,
           own, pair_out, pair_in, opp_out, opp_in, near_out, near_in, keep, fin0, tiles, got, acc,
           cell_sem, code_sem, grad_sem, pair_send, pair_recv,
           opp_send, opp_recv, near_send, near_recv, tile_send, tile_recv):
    dp = lax.axis_index("dp")
    group = lax.axis_index("table")
    x, c = lax.div(dp, 2), lax.rem(dp, 2)
    y, z = lax.div(group, NZ), lax.rem(group, NZ)
    pairs, tokens = cells.shape
    heads = scale_ref.shape[0]
    per = pairs // heads
    blocks = tokens // BLOCK
    partner = (x * 2 + 1 - c, group)
    ahead = (lax.rem(x + 1, NX) * 2 + c, group)
    behind = (lax.rem(x + NX - 1, NX) * 2 + c, group)
    sides = (ahead, behind)

    def dz_of(s):
        zz = lax.rem(s, NZ)
        odd = lax.rem(zz, 2)
        return lax.rem(NZ // 2 + (1 - 2 * odd) * lax.div(zz + 1, 2), NZ)

    def z_of(s):
        return lax.rem(z + dz_of(s), NZ)

    def source_of(s, i):
        return i * NZ + lax.rem(z + NZ - dz_of(s), NZ)

    def block_start(b):
        return pl.multiple_of(b * BLOCK, BLOCK)

    barrier = pltpu.get_barrier_semaphore()

    def greet(k, carry):
        pl.semaphore_signal(
            barrier, inc=1, device_id=(dp, lax.rem(group + k, NY * NZ)), device_id_type=MESH
        )
        return carry

    def cell_copy(b):
        cut = pl.ds(block_start(b), BLOCK)
        return pltpu.make_async_copy(cells_hbm.at[:, cut], cells.at[:, cut], cell_sem.at[b])

    def code_copy(b):
        cut = pl.ds(block_start(b), BLOCK)
        return pltpu.make_async_copy(codes_hbm.at[:, cut], codes.at[:, cut], code_sem.at[b])

    def grad_copy(b):
        cut = pl.ds(block_start(b), BLOCK)
        return pltpu.make_async_copy(grad_hbm.at[cut, :], grad.at[cut, :], grad_sem.at[b])

    for b in range(blocks):
        cell_copy(b).start()
        code_copy(b).start()
        grad_copy(b).start()
    for peer in (partner, ahead, behind):
        pl.semaphore_signal(barrier, inc=1, device_id=peer, device_id_type=MESH)
    lax.fori_loop(1, NY * NZ, greet, 0)
    acc[...] = jnp.zeros_like(acc)

    def pair_copy(q):
        return pltpu.make_async_remote_copy(
            src_ref=pair_out.at[q], dst_ref=pair_in.at[q],
            send_sem=pair_send.at[q], recv_sem=pair_recv.at[q],
            device_id=partner, device_id_type=MESH,
        )

    def opp_copy(q, side):
        return pltpu.make_async_remote_copy(
            src_ref=opp_out.at[q, side], dst_ref=opp_in.at[q, side],
            send_sem=opp_send.at[q, side], recv_sem=opp_recv.at[q, side],
            device_id=sides[side], device_id_type=MESH,
        )

    def near_copy(q, side, part):
        return pltpu.make_async_remote_copy(
            src_ref=near_out.at[q, side, part], dst_ref=near_in.at[q, side, part],
            send_sem=near_send.at[q, side, part], recv_sem=near_recv.at[q, side, part],
            device_id=sides[side], device_id_type=MESH,
        )

    def tile_copy(s, i):
        return pltpu.make_async_remote_copy(
            src_ref=tiles.at[s, i], dst_ref=got.at[s, y],
            send_sem=tile_send.at[s, i], recv_sem=tile_recv.at[s, y],
            device_id=(dp, i * NZ + z_of(s)), device_id_type=MESH,
        )

    def tile_arrival(s, i):
        return pltpu.make_async_remote_copy(
            src_ref=tiles.at[s, i], dst_ref=got.at[s, i],
            send_sem=tile_send.at[s, i], recv_sem=tile_recv.at[s, i],
            device_id=(dp, i * NZ + z_of(s)), device_id_type=MESH,
        )

    def stays(s, i):
        return (dz_of(s) == 0) & (y == i)

    def prepare(b):
        cell_copy(b).wait()
        code_copy(b).wait()
        cut = pl.ds(block_start(b), BLOCK)
        cell = cells[:, cut]
        row_of[cut, :] = (cell & (ROWS - 1)).astype(F32).astype(BF).T
        tile_of_pair[cut, :] = (cell >> 7).astype(F32).astype(BF).T
        weight = jnp.concatenate(
            [
                codes[h * per : (h + 1) * per, cut].astype(F32) * (scale_ref[h] / 128.0)
                for h in range(heads)
            ],
            axis=0,
        )
        weight_of[cut, :] = weight.astype(BF).T
        grad_copy(b).wait()
        for k in range(2 * NX):
            core = (1 - c) if k < NX else c
            block = lax.rem(x + k % NX, NX) * 2 + core
            columns = pl.ds(pl.multiple_of(block * ROWS, ROWS), ROWS)
            grads[k * ROWS : (k + 1) * ROWS, cut] = grad[cut, columns].T

    row_iota = lax.broadcasted_iota(jnp.int32, (PART, pairs), 0).astype(F32).astype(BF)
    tile_iota = lax.broadcasted_iota(jnp.int32, (TOUCH, pairs), 0).astype(F32).astype(BF)
    one = jnp.ones((), BF)
    zero = jnp.zeros((), BF)

    def coefficients(t):
        part = lax.div(t, blocks)
        start = block_start(lax.rem(t, blocks))
        shift = (part * PART).astype(F32).astype(BF)
        for v in range(BLOCK // 16):
            sixteen = pl.ds(pl.multiple_of(start + v * 16, 16), 16)
            row = row_of[sixteen, :] - shift
            tile = tile_of_pair[sixteen, :]
            weights = weight_of[sixteen, :]
            for u in range(16):
                row_hot = jnp.where(
                    jnp.broadcast_to(row[u : u + 1, :], (PART, pairs)) == row_iota, one, zero
                ).astype(jnp.float8_e4m3fn)
                tile_hot = jnp.where(
                    jnp.broadcast_to(tile[u : u + 1, :], (TOUCH, pairs)) == tile_iota,
                    jnp.broadcast_to(weights[u : u + 1, :], (TOUCH, pairs)),
                    zero,
                )
                result = lax.dot_general(
                    tile_hot, row_hot, (((1,), (1,)), ((), ())), preferred_element_type=F32
                )
                table[pl.ds(v * 16 + u, PAIRED, stride=STRIDE), :] = jnp.concatenate(
                    [result[k * PAIRED : (k + 1) * PAIRED] for k in range(PARTS)], axis=1
                )
        for j in range(PAIRED):
            coefs[part * PAIRED + j, pl.ds(start, BLOCK), :] = table[
                j * STRIDE : j * STRIDE + BLOCK, :
            ].astype(BF)

    def product(s, which):
        first = lax.div(s, NZ) * PAIRED + z_of(s)
        operand = jnp.concatenate([coefs[first], coefs[first + NZ]], axis=1)
        return jnp.dot(
            grads[which * NX * ROWS : (which + 1) * NX * ROWS, :], operand,
            preferred_element_type=F32,
        )

    def stage1(s):
        theirs = product(s, 0).astype(BF)
        for r in range(NX):
            for i in range(2):
                pair_out[s, r, i] = theirs[r * ROWS : (r + 1) * ROWS, i * ROWS : (i + 1) * ROWS]

        @pl.when(s == 0)
        def _():
            pl.semaphore_wait(barrier, NY * NZ + 2)

        pair_copy(s).start()
        mine = product(s, 1)
        slot = lax.rem(s, 2)
        for r in range(NX):
            for i in range(2):
                own[slot, r, i] = mine[r * ROWS : (r + 1) * ROWS, i * ROWS : (i + 1) * ROWS]

    def stage2(q):
        pair_copy(q).wait_recv()
        slot = lax.rem(q, 2)
        four = lax.rem(q, 4)

        def summed(r, i):
            return own[slot, r, i] + pair_in[q, r, i].astype(F32)

        for side in range(2):
            opp_out[q, side] = summed(2, side).astype(BF)
            opp_copy(q, side).start()
        for side in range(2):
            r = 1 if side == 0 else NX - 1
            near_out[q, side, 0] = summed(r, 1 - side).astype(BF)
            near_copy(q, side, 0).start()
        for side in range(2):
            r = 1 if side == 0 else NX - 1
            keep[slot, side] = summed(r, side)
        for i in range(2):
            fin0[four, i] = summed(0, i)

    def stage3(q):
        slot = lax.rem(q, 2)
        for side in range(2):
            opp_copy(q, side).wait_recv()
            near_out[q, side, 1] = (keep[slot, side] + opp_in[q, side].astype(F32)).astype(BF)
            near_copy(q, side, 1).start()

    def stage4(q):
        four = lax.rem(q, 4)
        for side in range(2):
            for part in range(2):
                near_copy(q, side, part).wait_recv()
        for i in range(2):
            total = fin0[four, i]
            for side in range(2):
                total = total + near_in[q, side, 1 if side == i else 0].astype(F32)
            total = total.T.astype(BF)
            for k in range(PARTS):
                tiles[q, i + 2 * k] = total[k * PART : (k + 1) * PART]
        for i in range(NY):
            @pl.when(jnp.logical_not(stays(q, i)))
            def _():
                tile_copy(q, i).start()

    def gather(s):
        for i in range(NY):
            @pl.when(jnp.logical_not(stays(s, i)))
            def _():
                tile_arrival(s, i).wait_recv()

            @pl.when(stays(s, i))
            def _():
                got[s, i] = tiles[s, i]

        slots = [slots_ref[source_of(s, i), group] for i in range(NY)]
        parts = [got[s, i].astype(F32) for i in range(NY)]
        half = lax.div(s, NZ)
        for k in range(OWN):
            total = acc[k, half]
            for i in range(NY):
                total = total + jnp.where(slots[i] == k, parts[i], 0.0)
            acc[k, half] = total

    lag = 6

    def step(t, carry):
        s = t - blocks
        pl.when(t < blocks)(lambda: prepare(t))
        pl.when((s >= 0) & (s < STEPS))(lambda: stage1(s))
        pl.when(t < PARTS * blocks)(lambda: coefficients(t))
        pl.when((s >= 1) & (s < STEPS + 1))(lambda: stage2(s - 1))
        pl.when((s >= 2) & (s < STEPS + 2))(lambda: stage3(s - 2))
        pl.when((s >= 3) & (s < STEPS + 3))(lambda: stage4(s - 3))
        pl.when(s >= lag)(lambda: gather(s - lag))
        return carry

    lax.fori_loop(0, blocks + STEPS + lag, step, 0)

    for k in range(OWN):
        for h in range(PARTS):
            out_ref[k * ROWS + h * PART : k * ROWS + (h + 1) * PART, :] = acc[k, h].astype(BF)

    def drain(q, carry):
        pair_copy(q).wait_send()
        for side in range(2):
            opp_copy(q, side).wait_send()
            for part in range(2):
                near_copy(q, side, part).wait_send()
        for i in range(NY):
            @pl.when(jnp.logical_not(stays(q, i)))
            def _():
                tile_arrival(q, i).wait_send()
        return carry

    lax.fori_loop(0, STEPS, drain, 0)


def body(out_grad, pair_cells, weight_codes, head_scale, touch_slots):
    tokens, width = out_grad.shape
    pairs = pair_cells.shape[1] * pair_cells.shape[2]
    cells = pair_cells.transpose(1, 2, 0).reshape(pairs, tokens)
    codes = weight_codes.transpose(1, 2, 0).reshape(pairs, tokens)
    blocks = tokens // BLOCK
    square = (ROWS, ROWS)
    piece = (PART, ROWS)
    dma = pltpu.SemaphoreType.DMA
    smem = pl.BlockSpec(memory_space=pltpu.SMEM)
    hbm = pl.BlockSpec(memory_space=pltpu.HBM)
    return pl.pallas_call(
        kernel,
        in_specs=[smem, smem, hbm, hbm, hbm],
        out_specs=pl.BlockSpec(memory_space=pltpu.VMEM),
        out_shape=jax.ShapeDtypeStruct((OWN * ROWS, ROWS), BF),
        scratch_shapes=[
            pltpu.VMEM((pairs, tokens), jnp.int32),
            pltpu.VMEM((pairs, tokens), jnp.int32),
            pltpu.VMEM((tokens, width), BF),
            pltpu.VMEM((tokens, pairs), BF),
            pltpu.VMEM((tokens, pairs), BF),
            pltpu.VMEM((tokens, pairs), BF),
            pltpu.VMEM((PAIRED * STRIDE, ROWS), F32),
            pltpu.VMEM((PARTS * PAIRED, tokens, ROWS), BF),
            pltpu.VMEM((width, tokens), BF),
            pltpu.VMEM((2, NX, 2) + square, F32),
            pltpu.VMEM((STEPS, NX, 2) + square, BF),
            pltpu.VMEM((STEPS, NX, 2) + square, BF),
            pltpu.VMEM((STEPS, 2) + square, BF),
            pltpu.VMEM((STEPS, 2) + square, BF),
            pltpu.VMEM((STEPS, 2, 2) + square, BF),
            pltpu.VMEM((STEPS, 2, 2) + square, BF),
            pltpu.VMEM((2, 2) + square, F32),
            pltpu.VMEM((4, 2) + square, F32),
            pltpu.VMEM((STEPS, NY) + piece, BF),
            pltpu.VMEM((STEPS, NY) + piece, BF),
            pltpu.VMEM((OWN, PARTS) + piece, F32),
            dma((blocks,)),
            dma((blocks,)),
            dma((blocks,)),
            dma((STEPS,)),
            dma((STEPS,)),
            dma((STEPS, 2)),
            dma((STEPS, 2)),
            dma((STEPS, 2, 2)),
            dma((STEPS, 2, 2)),
            dma((STEPS, NY)),
            dma((STEPS, NY)),
        ],
        compiler_params=pltpu.CompilerParams(
            collective_id=0, has_side_effects=True, vmem_limit_bytes=60 << 20
        ),
        name="value_grad",
    )(head_scale, touch_slots.reshape(touch_slots.shape[0], -1), cells, codes, out_grad)


def solution(mesh):
    return jax.shard_map(
        body,
        mesh=mesh,
        in_specs=(
            P(("dp", "table"), None),
            P(("dp", "table"), None, None),
            P(("dp", "table"), None, None),
            P(),
            P(),
        ),
        out_specs=P("table", "dp"),
        check_vma=False,
    )
```

```python
import functools

import jax
import jax.numpy as jnp
from jax import lax
from jax.experimental import pallas as pl
from jax.experimental.pallas import tpu as pltpu
from jax.sharding import PartitionSpec as P

ROWS = 128
TOUCH = 32
OWN = 8
NX = 4
NY = 4
NZ = 8
PARTS = 2
PART = ROWS // PARTS
PAIRED = TOUCH // PARTS
BLOCK = 128
STRIDE = BLOCK + 8
STEPS = PARTS * NZ // 2
SPAN = 4
HALF = SPAN // 2
LAG3 = 2
LAG4 = 3
LAG5 = 8
MESH = pl.DeviceIdType.MESH
BF = jnp.bfloat16
F32 = jnp.float32


def kernel(scale_ref, slots_ref, cells_hbm, codes_hbm, grad_hbm, out_ref,
           cells, codes, grad, row_of, tile_of_pair, weight_of, table, coefs, grads,
           own, pair_out, pair_in, opp_out, opp_in, near_out, near_in, keep, fin0, tiles, got, acc,
           cell_sem, code_sem, grad_sem, pair_send, pair_recv,
           opp_send, opp_recv, near_send, near_recv, tile_send, tile_recv):
    dp = lax.axis_index("dp")
    group = lax.axis_index("table")
    x, c = lax.div(dp, 2), lax.rem(dp, 2)
    y, z = lax.div(group, NZ), lax.rem(group, NZ)
    pairs, tokens = cells.shape
    heads = scale_ref.shape[0]
    per = pairs // heads
    blocks = tokens // BLOCK
    partner = (x * 2 + 1 - c, group)
    ahead = (lax.rem(x + 1, NX) * 2 + c, group)
    behind = (lax.rem(x + NX - 1, NX) * 2 + c, group)
    sides = (ahead, behind)

    def dz_of(s, i):
        far = lax.rem(s, NZ // 2)
        return lax.rem(NZ // 2 + far if i == 0 else NZ // 2 - 1 - far, NZ)

    def z_of(s, i):
        return lax.rem(z + dz_of(s, i), NZ)

    def source_of(s, i, k):
        return k * NZ + lax.rem(z + NZ - dz_of(s, i), NZ)

    def block_start(b):
        return pl.multiple_of(b * BLOCK, BLOCK)

    barrier = pltpu.get_barrier_semaphore()

    def greet(k, carry):
        pl.semaphore_signal(
            barrier, inc=1, device_id=(dp, lax.rem(group + k, NY * NZ)), device_id_type=MESH
        )
        return carry

    def cell_copy(b):
        cut = pl.ds(block_start(b), BLOCK)
        return pltpu.make_async_copy(cells_hbm.at[:, cut], cells.at[:, cut], cell_sem.at[b])

    def code_copy(b):
        cut = pl.ds(block_start(b), BLOCK)
        return pltpu.make_async_copy(codes_hbm.at[:, cut], codes.at[:, cut], code_sem.at[b])

    def grad_copy(b):
        cut = pl.ds(block_start(b), BLOCK)
        return pltpu.make_async_copy(grad_hbm.at[cut, :], grad.at[cut, :], grad_sem.at[b])

    for b in range(blocks):
        cell_copy(b).start()
        code_copy(b).start()
        grad_copy(b).start()
    for peer in (partner, ahead, behind):
        pl.semaphore_signal(barrier, inc=1, device_id=peer, device_id_type=MESH)
    lax.fori_loop(1, NY * NZ, greet, 0)
    acc[...] = jnp.zeros_like(acc)

    def pair_copy(q):
        return pltpu.make_async_remote_copy(
            src_ref=pair_out.at[q], dst_ref=pair_in.at[q],
            send_sem=pair_send.at[q], recv_sem=pair_recv.at[q],
            device_id=partner, device_id_type=MESH,
        )

    def opp_copy(q, side):
        return pltpu.make_async_remote_copy(
            src_ref=opp_out.at[q, side], dst_ref=opp_in.at[q, side],
            send_sem=opp_send.at[q, side], recv_sem=opp_recv.at[q, side],
            device_id=sides[side], device_id_type=MESH,
        )

    def near_copy(q, side, part):
        return pltpu.make_async_remote_copy(
            src_ref=near_out.at[q, side, part], dst_ref=near_in.at[q, side, part],
            send_sem=near_send.at[q, side, part], recv_sem=near_recv.at[q, side, part],
            device_id=sides[side], device_id_type=MESH,
        )

    def tile_copy(s, i, k):
        return pltpu.make_async_remote_copy(
            src_ref=tiles.at[s, i, k], dst_ref=got.at[s, i, y],
            send_sem=tile_send.at[s, i, k], recv_sem=tile_recv.at[s, i, y],
            device_id=(dp, k * NZ + z_of(s, i)), device_id_type=MESH,
        )

    def tile_arrival(s, i, k):
        return pltpu.make_async_remote_copy(
            src_ref=tiles.at[s, i, k], dst_ref=got.at[s, i, k],
            send_sem=tile_send.at[s, i, k], recv_sem=tile_recv.at[s, i, k],
            device_id=(dp, k * NZ + z_of(s, i)), device_id_type=MESH,
        )

    def stays(s, i, k):
        return (dz_of(s, i) == 0) & (y == k)

    def prepare(b):
        cell_copy(b).wait()
        code_copy(b).wait()
        cut = pl.ds(block_start(b), BLOCK)
        cell = cells[:, cut]
        row_of[cut, :] = (cell & (ROWS - 1)).astype(F32).astype(BF).T
        tile_of_pair[cut, :] = (cell >> 7).astype(F32).astype(BF).T
        weight = jnp.concatenate(
            [
                codes[h * per : (h + 1) * per, cut].astype(F32) * (scale_ref[h] / 128.0)
                for h in range(heads)
            ],
            axis=0,
        )
        weight_of[cut, :] = weight.astype(BF).T
        grad_copy(b).wait()
        for k in range(2 * NX):
            core = (1 - c) if k < NX else c
            block = lax.rem(x + k % NX, NX) * 2 + core
            columns = pl.ds(pl.multiple_of(block * ROWS, ROWS), ROWS)
            grads[k * ROWS : (k + 1) * ROWS, cut] = grad[cut, columns].T

    row_iota = lax.broadcasted_iota(jnp.int32, (PART, pairs), 0).astype(F32).astype(BF)
    tile_iota = lax.broadcasted_iota(jnp.int32, (TOUCH, pairs), 0).astype(F32).astype(BF)
    one = jnp.ones((), BF)
    zero = jnp.zeros((), BF)

    def coefficients(t):
        part = lax.div(t, blocks)
        start = block_start(lax.rem(t, blocks))
        shift = (part * PART).astype(F32).astype(BF)
        for v in range(BLOCK // 16):
            sixteen = pl.ds(pl.multiple_of(start + v * 16, 16), 16)
            row = row_of[sixteen, :] - shift
            tile = tile_of_pair[sixteen, :]
            weights = weight_of[sixteen, :]
            for u in range(16):
                row_hot = jnp.where(
                    jnp.broadcast_to(row[u : u + 1, :], (PART, pairs)) == row_iota, one, zero
                ).astype(jnp.float8_e4m3fn)
                tile_hot = jnp.where(
                    jnp.broadcast_to(tile[u : u + 1, :], (TOUCH, pairs)) == tile_iota,
                    jnp.broadcast_to(weights[u : u + 1, :], (TOUCH, pairs)),
                    zero,
                )
                result = lax.dot_general(
                    tile_hot, row_hot, (((1,), (1,)), ((), ())), preferred_element_type=F32
                )
                table[pl.ds(v * 16 + u, PAIRED, stride=STRIDE), :] = jnp.concatenate(
                    [result[k * PAIRED : (k + 1) * PAIRED] for k in range(PARTS)], axis=1
                )
        for j in range(PAIRED):
            coefs[part * PAIRED + j, pl.ds(start, BLOCK), :] = table[
                j * STRIDE : j * STRIDE + BLOCK, :
            ].astype(BF)

    def product(s, which):
        part = lax.div(s, NZ // 2) * PAIRED
        operand = jnp.concatenate(
            [coefs[part + a * NZ + z_of(s, i)] for i in range(2) for a in range(2)], axis=1
        )
        return jnp.dot(
            grads[which * NX * ROWS : (which + 1) * NX * ROWS, :], operand,
            preferred_element_type=F32,
        )

    def stage1(s):
        theirs = product(s, 0).astype(BF)
        for r in range(NX):
            for i in range(SPAN):
                pair_out[s, r, i] = theirs[r * ROWS : (r + 1) * ROWS, i * ROWS : (i + 1) * ROWS]

        @pl.when(s == 0)
        def _():
            pl.semaphore_wait(barrier, NY * NZ + 2)

        pair_copy(s).start()
        mine = product(s, 1)
        slot = lax.rem(s, 2)
        for r in range(NX):
            for i in range(SPAN):
                own[slot, r, i] = mine[r * ROWS : (r + 1) * ROWS, i * ROWS : (i + 1) * ROWS]

    def stage2(q):
        pair_copy(q).wait_recv()
        slot = lax.rem(q, 2)

        def summed(r, half):
            lo = half * HALF
            return own[slot, r, lo : lo + HALF] + pair_in[q, r, lo : lo + HALF].astype(F32)

        for side in range(2):
            opp_out[q, side] = summed(2, side).astype(BF)
            opp_copy(q, side).start()
        for side in range(2):
            r = 1 if side == 0 else NX - 1
            near_out[q, side, 0] = summed(r, 1 - side).astype(BF)
            near_copy(q, side, 0).start()
        for side in range(2):
            r = 1 if side == 0 else NX - 1
            keep[lax.rem(q, 4), side] = summed(r, side)
        for half in range(2):
            fin0[lax.rem(q, 8), half] = summed(0, half)

    def stage3(q):
        slot = lax.rem(q, 4)
        for side in range(2):
            opp_copy(q, side).wait_recv()
            near_out[q, side, 1] = (keep[slot, side] + opp_in[q, side].astype(F32)).astype(BF)
            near_copy(q, side, 1).start()

    def stage4(q):
        eight = lax.rem(q, 8)
        for side in range(2):
            for part in range(2):
                near_copy(q, side, part).wait_recv()
        for i in range(2):
            total = fin0[eight, i]
            for side in range(2):
                total = total + near_in[q, side, 1 if side == i else 0].astype(F32)
            for a in range(HALF):
                turned = total[a].T.astype(BF)
                for k in range(PARTS):
                    tiles[q, i, a + HALF * k] = turned[k * PART : (k + 1) * PART]
            for k in range(NY):
                @pl.when(jnp.logical_not(stays(q, i, k)))
                def _():
                    tile_copy(q, i, k).start()

    def gather(s):
        for i in range(2):
            for k in range(NY):
                @pl.when(jnp.logical_not(stays(s, i, k)))
                def _():
                    tile_arrival(s, i, k).wait_recv()

                @pl.when(stays(s, i, k))
                def _():
                    got[s, i, k] = tiles[s, i, k]

        pieces = [(i, k) for i in range(2) for k in range(NY)]
        slots = [slots_ref[source_of(s, i, k), group] for i, k in pieces]
        parts = [got[s, i, k].astype(F32) for i, k in pieces]
        part = lax.div(s, NZ // 2)
        for o in range(OWN):
            total = acc[o, part]
            for slot, value in zip(slots, parts):
                total = total + jnp.where(slot == o, value, 0.0)
            acc[o, part] = total

    def more(s):
        def one_block(half, carry):
            coefficients(blocks + half)
            return carry

        lax.fori_loop(3 * (s - 1), lax.min(3 * s, blocks), one_block, 0)

    def step(t, carry):
        s = t - blocks
        pl.when(t < blocks)(lambda: prepare(t))
        pl.when((s >= 0) & (s < STEPS))(lambda: stage1(s))
        pl.when(t < blocks)(lambda: coefficients(t))
        pl.when((s >= 1) & (s < STEPS + 1))(lambda: stage2(s - 1))
        pl.when((s >= LAG3) & (s < STEPS + LAG3))(lambda: stage3(s - LAG3))
        pl.when((s >= LAG4) & (s < STEPS + LAG4))(lambda: stage4(s - LAG4))
        pl.when(s >= LAG5)(lambda: gather(s - LAG5))
        pl.when((s >= 1) & (s < 4))(lambda: more(s))
        return carry

    lax.fori_loop(0, blocks + STEPS + LAG5, step, 0)

    for k in range(OWN):
        for h in range(PARTS):
            out_ref[k * ROWS + h * PART : k * ROWS + (h + 1) * PART, :] = acc[k, h].astype(BF)

    def drain(q, carry):
        pair_copy(q).wait_send()
        for side in range(2):
            opp_copy(q, side).wait_send()
            for part in range(2):
                near_copy(q, side, part).wait_send()
        for i in range(2):
            for k in range(NY):
                @pl.when(jnp.logical_not(stays(q, i, k)))
                def _():
                    tile_arrival(q, i, k).wait_send()
        return carry

    lax.fori_loop(0, STEPS, drain, 0)


def body(out_grad, pair_cells, weight_codes, head_scale, touch_slots):
    tokens, width = out_grad.shape
    pairs = pair_cells.shape[1] * pair_cells.shape[2]
    cells = pair_cells.transpose(1, 2, 0).reshape(pairs, tokens)
    codes = weight_codes.transpose(1, 2, 0).reshape(pairs, tokens)
    blocks = tokens // BLOCK
    square = (ROWS, ROWS)
    piece = (PART, ROWS)
    dma = pltpu.SemaphoreType.DMA
    smem = pl.BlockSpec(memory_space=pltpu.SMEM)
    hbm = pl.BlockSpec(memory_space=pltpu.HBM)
    return pl.pallas_call(
        kernel,
        in_specs=[smem, smem, hbm, hbm, hbm],
        out_specs=pl.BlockSpec(memory_space=pltpu.VMEM),
        out_shape=jax.ShapeDtypeStruct((OWN * ROWS, ROWS), BF),
        scratch_shapes=[
            pltpu.VMEM((pairs, tokens), jnp.int32),
            pltpu.VMEM((pairs, tokens), jnp.int32),
            pltpu.VMEM((tokens, width), BF),
            pltpu.VMEM((tokens, pairs), BF),
            pltpu.VMEM((tokens, pairs), BF),
            pltpu.VMEM((tokens, pairs), BF),
            pltpu.VMEM((PAIRED * STRIDE, ROWS), F32),
            pltpu.VMEM((PARTS * PAIRED, tokens, ROWS), BF),
            pltpu.VMEM((width, tokens), BF),
            pltpu.VMEM((2, NX, SPAN) + square, F32),
            pltpu.VMEM((STEPS, NX, SPAN) + square, BF),
            pltpu.VMEM((STEPS, NX, SPAN) + square, BF),
            pltpu.VMEM((STEPS, 2, HALF) + square, BF),
            pltpu.VMEM((STEPS, 2, HALF) + square, BF),
            pltpu.VMEM((STEPS, 2, 2, HALF) + square, BF),
            pltpu.VMEM((STEPS, 2, 2, HALF) + square, BF),
            pltpu.VMEM((4, 2, HALF) + square, F32),
            pltpu.VMEM((8, 2, HALF) + square, F32),
            pltpu.VMEM((STEPS, 2, NY) + piece, BF),
            pltpu.VMEM((STEPS, 2, NY) + piece, BF),
            pltpu.VMEM((OWN, PARTS) + piece, F32),
            dma((blocks,)),
            dma((blocks,)),
            dma((blocks,)),
            dma((STEPS,)),
            dma((STEPS,)),
            dma((STEPS, 2)),
            dma((STEPS, 2)),
            dma((STEPS, 2, 2)),
            dma((STEPS, 2, 2)),
            dma((STEPS, 2, NY)),
            dma((STEPS, 2, NY)),
        ],
        compiler_params=pltpu.CompilerParams(
            collective_id=0, has_side_effects=True, vmem_limit_bytes=60 << 20
        ),
        name="value_grad",
    )(head_scale, touch_slots.reshape(touch_slots.shape[0], -1), cells, codes, out_grad)


def solution(mesh):
    return jax.shard_map(
        body,
        mesh=mesh,
        in_specs=(
            P(("dp", "table"), None),
            P(("dp", "table"), None, None),
            P(("dp", "table"), None, None),
            P(),
            P(),
        ),
        out_specs=P("table", "dp"),
        check_vma=False,
    )
```

```python
import functools

import jax
import jax.numpy as jnp
from jax import lax
from jax.experimental import pallas as pl
from jax.experimental.pallas import tpu as pltpu
from jax.sharding import PartitionSpec as P

ROWS = 128
TOUCH = 32
OWN = 8
NX = 4
NY = 4
NZ = 8
PARTS = 2
PART = ROWS // PARTS
PAIRED = TOUCH // PARTS
BLOCK = 128
STRIDE = BLOCK + 8
STEPS = PARTS * NZ // 2
SPAN = 4
HALF = SPAN // 2
LAG3 = 2
LAG4 = 3
LAG5 = 8
MESH = pl.DeviceIdType.MESH
BF = jnp.bfloat16
F32 = jnp.float32


def kernel(scale_ref, slots_ref, cells_hbm, codes_hbm, grad_hbm, out_ref,
           cells, codes, grad, row_of, tile_of_pair, weight_of, table, coefs, grads,
           own, pair_out, pair_in, opp_out, opp_in, near_out, near_in, keep, fin0, tiles, got, acc,
           cell_sem, code_sem, grad_sem, pair_send, pair_recv,
           opp_send, opp_recv, near_send, near_recv, tile_send, tile_recv):
    dp = lax.axis_index("dp")
    group = lax.axis_index("table")
    x, c = lax.div(dp, 2), lax.rem(dp, 2)
    y, z = lax.div(group, NZ), lax.rem(group, NZ)
    pairs, tokens = cells.shape
    heads = scale_ref.shape[0]
    per = pairs // heads
    blocks = tokens // BLOCK
    partner = (x * 2 + 1 - c, group)
    ahead = (lax.rem(x + 1, NX) * 2 + c, group)
    behind = (lax.rem(x + NX - 1, NX) * 2 + c, group)
    sides = (ahead, behind)

    def dz_of(s, i):
        far = lax.rem(s, NZ // 2)
        return lax.rem(NZ // 2 + far if i == 0 else NZ // 2 - 1 - far, NZ)

    def z_of(s, i):
        return lax.rem(z + dz_of(s, i), NZ)

    def source_of(s, i, k):
        return k * NZ + lax.rem(z + NZ - dz_of(s, i), NZ)

    def block_start(b):
        return pl.multiple_of(b * BLOCK, BLOCK)

    barrier = pltpu.get_barrier_semaphore()

    def greet(k, carry):
        pl.semaphore_signal(
            barrier, inc=1, device_id=(dp, lax.rem(group + k, NY * NZ)), device_id_type=MESH
        )
        return carry

    def cell_copy(b):
        cut = pl.ds(block_start(b), BLOCK)
        return pltpu.make_async_copy(cells_hbm.at[:, cut], cells.at[:, cut], cell_sem.at[b])

    def code_copy(b):
        cut = pl.ds(block_start(b), BLOCK)
        return pltpu.make_async_copy(codes_hbm.at[:, cut], codes.at[:, cut], code_sem.at[b])

    def grad_copy(b):
        cut = pl.ds(block_start(b), BLOCK)
        return pltpu.make_async_copy(grad_hbm.at[cut, :], grad.at[cut, :], grad_sem.at[b])

    for b in range(blocks):
        cell_copy(b).start()
        code_copy(b).start()
        grad_copy(b).start()
    for peer in (partner, ahead, behind):
        pl.semaphore_signal(barrier, inc=1, device_id=peer, device_id_type=MESH)
    lax.fori_loop(1, NY * NZ, greet, 0)
    acc[...] = jnp.zeros_like(acc)

    def pair_copy(q):
        return pltpu.make_async_remote_copy(
            src_ref=pair_out.at[q], dst_ref=pair_in.at[q],
            send_sem=pair_send.at[q], recv_sem=pair_recv.at[q],
            device_id=partner, device_id_type=MESH,
        )

    def opp_copy(q, side):
        return pltpu.make_async_remote_copy(
            src_ref=opp_out.at[q, side], dst_ref=opp_in.at[q, side],
            send_sem=opp_send.at[q, side], recv_sem=opp_recv.at[q, side],
            device_id=sides[side], device_id_type=MESH,
        )

    def near_copy(q, side, part):
        return pltpu.make_async_remote_copy(
            src_ref=near_out.at[q, side, part], dst_ref=near_in.at[q, side, part],
            send_sem=near_send.at[q, side, part], recv_sem=near_recv.at[q, side, part],
            device_id=sides[side], device_id_type=MESH,
        )

    def tile_copy(s, i, k):
        return pltpu.make_async_remote_copy(
            src_ref=tiles.at[s, i, k], dst_ref=got.at[s, i, y],
            send_sem=tile_send.at[s, i, k], recv_sem=tile_recv.at[s, i, y],
            device_id=(dp, k * NZ + z_of(s, i)), device_id_type=MESH,
        )

    def tile_arrival(s, i, k):
        return pltpu.make_async_remote_copy(
            src_ref=tiles.at[s, i, k], dst_ref=got.at[s, i, k],
            send_sem=tile_send.at[s, i, k], recv_sem=tile_recv.at[s, i, k],
            device_id=(dp, k * NZ + z_of(s, i)), device_id_type=MESH,
        )

    def stays(s, i, k):
        return (dz_of(s, i) == 0) & (y == k)

    def prepare(b):
        cell_copy(b).wait()
        code_copy(b).wait()
        cut = pl.ds(block_start(b), BLOCK)
        cell = cells[:, cut]
        row_of[cut, :] = (cell & (ROWS - 1)).astype(F32).astype(BF).T
        tile_of_pair[cut, :] = (cell >> 7).astype(F32).astype(BF).T
        weight = jnp.concatenate(
            [
                codes[h * per : (h + 1) * per, cut].astype(F32) * (scale_ref[h] / 128.0)
                for h in range(heads)
            ],
            axis=0,
        )
        weight_of[cut, :] = weight.astype(BF).T
        grad_copy(b).wait()
        for k in range(2 * NX):
            core = (1 - c) if k < NX else c
            block = lax.rem(x + k % NX, NX) * 2 + core
            columns = pl.ds(pl.multiple_of(block * ROWS, ROWS), ROWS)
            grads[k * ROWS : (k + 1) * ROWS, cut] = grad[cut, columns].T

    row_iota = lax.broadcasted_iota(jnp.int32, (PART, pairs), 0).astype(F32).astype(BF)
    tile_iota = lax.broadcasted_iota(jnp.int32, (TOUCH, pairs), 0).astype(F32).astype(BF)
    one = jnp.ones((), BF)
    zero = jnp.zeros((), BF)

    def coefficients(t):
        part = lax.div(t, blocks)
        start = block_start(lax.rem(t, blocks))
        shift = (part * PART).astype(F32).astype(BF)
        for v in range(BLOCK // 16):
            sixteen = pl.ds(pl.multiple_of(start + v * 16, 16), 16)
            row = row_of[sixteen, :] - shift
            tile = tile_of_pair[sixteen, :]
            weights = weight_of[sixteen, :]
            for u in range(16):
                row_hot = jnp.where(
                    jnp.broadcast_to(row[u : u + 1, :], (PART, pairs)) == row_iota, one, zero
                ).astype(jnp.float8_e4m3fn)
                tile_hot = jnp.where(
                    jnp.broadcast_to(tile[u : u + 1, :], (TOUCH, pairs)) == tile_iota,
                    jnp.broadcast_to(weights[u : u + 1, :], (TOUCH, pairs)),
                    zero,
                )
                result = lax.dot_general(
                    tile_hot, row_hot, (((1,), (1,)), ((), ())), preferred_element_type=F32
                )
                table[pl.ds(v * 16 + u, PAIRED, stride=STRIDE), :] = jnp.concatenate(
                    [result[k * PAIRED : (k + 1) * PAIRED] for k in range(PARTS)], axis=1
                )
        for j in range(PAIRED):
            coefs[part * PAIRED + j, pl.ds(start, BLOCK), :] = table[
                j * STRIDE : j * STRIDE + BLOCK, :
            ].astype(BF)

    def product(s, which):
        part = lax.div(s, NZ // 2) * PAIRED
        operand = jnp.concatenate(
            [coefs[part + a * NZ + z_of(s, i)] for i in range(2) for a in range(2)], axis=1
        )
        return jnp.dot(
            grads[which * NX * ROWS : (which + 1) * NX * ROWS, :], operand,
            preferred_element_type=F32,
        )

    def stage1(s):
        theirs = product(s, 0).astype(BF)
        for r in range(NX):
            for i in range(SPAN):
                pair_out[s, r, i] = theirs[r * ROWS : (r + 1) * ROWS, i * ROWS : (i + 1) * ROWS]

        @pl.when(s == 0)
        def _():
            pl.semaphore_wait(barrier, NY * NZ + 2)

        pair_copy(s).start()
        mine = product(s, 1)
        slot = lax.rem(s, 2)
        for r in range(NX):
            for i in range(SPAN):
                own[slot, r, i] = mine[r * ROWS : (r + 1) * ROWS, i * ROWS : (i + 1) * ROWS]

    def stage2(q):
        pair_copy(q).wait_recv()
        slot = lax.rem(q, 2)

        def summed(r, half):
            lo = half * HALF
            return own[slot, r, lo : lo + HALF] + pair_in[q, r, lo : lo + HALF].astype(F32)

        for side in range(2):
            opp_out[q, side] = summed(2, side).astype(BF)
            opp_copy(q, side).start()
        for side in range(2):
            r = 1 if side == 0 else NX - 1
            near_out[q, side, 0] = summed(r, 1 - side).astype(BF)
            near_copy(q, side, 0).start()
        for side in range(2):
            r = 1 if side == 0 else NX - 1
            keep[lax.rem(q, 4), side] = summed(r, side)
        for half in range(2):
            fin0[lax.rem(q, 8), half] = summed(0, half)

    def stage3(q):
        slot = lax.rem(q, 4)
        for side in range(2):
            opp_copy(q, side).wait_recv()
            near_out[q, side, 1] = (keep[slot, side] + opp_in[q, side].astype(F32)).astype(BF)
            near_copy(q, side, 1).start()

    def stage4(q):
        eight = lax.rem(q, 8)
        for side in range(2):
            for part in range(2):
                near_copy(q, side, part).wait_recv()
        for i in range(2):
            total = fin0[eight, i]
            for side in range(2):
                total = total + near_in[q, side, 1 if side == i else 0].astype(F32)
            for a in range(HALF):
                turned = total[a].T.astype(BF)
                for k in range(PARTS):
                    tiles[q, i, a + HALF * k] = turned[k * PART : (k + 1) * PART]
            for k in range(NY):
                @pl.when(jnp.logical_not(stays(q, i, k)))
                def _():
                    tile_copy(q, i, k).start()

    def gather(s):
        for i in range(2):
            for k in range(NY):
                @pl.when(jnp.logical_not(stays(s, i, k)))
                def _():
                    tile_arrival(s, i, k).wait_recv()

                @pl.when(stays(s, i, k))
                def _():
                    got[s, i, k] = tiles[s, i, k]

        pieces = [(i, k) for i in range(2) for k in range(NY)]
        slots = [slots_ref[source_of(s, i, k), group] for i, k in pieces]
        parts = [got[s, i, k].astype(F32) for i, k in pieces]
        part = lax.div(s, NZ // 2)
        for o in range(OWN):
            total = acc[o, part]
            for slot, value in zip(slots, parts):
                total = total + jnp.where(slot == o, value, 0.0)
            acc[o, part] = total

    def more(s):
        def one_block(half, carry):
            coefficients(blocks + half)
            return carry

        lax.fori_loop(3 * (s - 1), lax.min(3 * s, blocks), one_block, 0)

    def step(t, carry):
        s = t - blocks
        pl.when(t < blocks)(lambda: prepare(t))
        pl.when((s >= 0) & (s < STEPS))(lambda: stage1(s))
        pl.when(t < blocks)(lambda: coefficients(t))
        pl.when((s >= 1) & (s < STEPS + 1))(lambda: stage2(s - 1))
        pl.when((s >= LAG3) & (s < STEPS + LAG3))(lambda: stage3(s - LAG3))
        pl.when((s >= LAG4) & (s < STEPS + LAG4))(lambda: stage4(s - LAG4))
        pl.when(s >= LAG5)(lambda: gather(s - LAG5))
        pl.when((s >= 1) & (s < 4))(lambda: more(s))
        return carry

    lax.fori_loop(0, blocks + STEPS + LAG5, step, 0)

    for k in range(OWN):
        for h in range(PARTS):
            out_ref[k * ROWS + h * PART : k * ROWS + (h + 1) * PART, :] = acc[k, h].astype(BF)

    def drain(q, carry):
        pair_copy(q).wait_send()
        for side in range(2):
            opp_copy(q, side).wait_send()
            for part in range(2):
                near_copy(q, side, part).wait_send()
        for i in range(2):
            for k in range(NY):
                @pl.when(jnp.logical_not(stays(q, i, k)))
                def _():
                    tile_arrival(q, i, k).wait_send()
        return carry

    lax.fori_loop(0, STEPS, drain, 0)


def body(out_grad, pair_cells, weight_codes, head_scale, touch_slots):
    tokens, width = out_grad.shape
    pairs = pair_cells.shape[1] * pair_cells.shape[2]
    cells = pair_cells.transpose(1, 2, 0).reshape(pairs, tokens)
    codes = weight_codes.transpose(1, 2, 0).reshape(pairs, tokens)
    blocks = tokens // BLOCK
    square = (ROWS, ROWS)
    piece = (PART, ROWS)
    dma = pltpu.SemaphoreType.DMA
    smem = pl.BlockSpec(memory_space=pltpu.SMEM)
    hbm = pl.BlockSpec(memory_space=pltpu.HBM)
    operands = [
        pltpu.with_memory_space_constraint(array, pltpu.HBM)
        for array in (
            head_scale,
            touch_slots.reshape(touch_slots.shape[0], -1),
            cells,
            codes,
            out_grad,
        )
    ]
    return pl.pallas_call(
        kernel,
        in_specs=[smem, smem, hbm, hbm, hbm],
        out_specs=pl.BlockSpec(memory_space=pltpu.VMEM),
        out_shape=jax.ShapeDtypeStruct((OWN * ROWS, ROWS), BF),
        scratch_shapes=[
            pltpu.VMEM((pairs, tokens), jnp.int32),
            pltpu.VMEM((pairs, tokens), jnp.int32),
            pltpu.VMEM((tokens, width), BF),
            pltpu.VMEM((tokens, pairs), BF),
            pltpu.VMEM((tokens, pairs), BF),
            pltpu.VMEM((tokens, pairs), BF),
            pltpu.VMEM((PAIRED * STRIDE, ROWS), F32),
            pltpu.VMEM((PARTS * PAIRED, tokens, ROWS), BF),
            pltpu.VMEM((width, tokens), BF),
            pltpu.VMEM((2, NX, SPAN) + square, F32),
            pltpu.VMEM((STEPS, NX, SPAN) + square, BF),
            pltpu.VMEM((STEPS, NX, SPAN) + square, BF),
            pltpu.VMEM((STEPS, 2, HALF) + square, BF),
            pltpu.VMEM((STEPS, 2, HALF) + square, BF),
            pltpu.VMEM((STEPS, 2, 2, HALF) + square, BF),
            pltpu.VMEM((STEPS, 2, 2, HALF) + square, BF),
            pltpu.VMEM((4, 2, HALF) + square, F32),
            pltpu.VMEM((8, 2, HALF) + square, F32),
            pltpu.VMEM((STEPS, 2, NY) + piece, BF),
            pltpu.VMEM((STEPS, 2, NY) + piece, BF),
            pltpu.VMEM((OWN, PARTS) + piece, F32),
            dma((blocks,)),
            dma((blocks,)),
            dma((blocks,)),
            dma((STEPS,)),
            dma((STEPS,)),
            dma((STEPS, 2)),
            dma((STEPS, 2)),
            dma((STEPS, 2, 2)),
            dma((STEPS, 2, 2)),
            dma((STEPS, 2, NY)),
            dma((STEPS, 2, NY)),
        ],
        compiler_params=pltpu.CompilerParams(
            collective_id=0, has_side_effects=True, vmem_limit_bytes=45 << 20
        ),
        name="value_grad",
    )(*operands)


def solution(mesh):
    return jax.shard_map(
        body,
        mesh=mesh,
        in_specs=(
            P(("dp", "table"), None),
            P(("dp", "table"), None, None),
            P(("dp", "table"), None, None),
            P(),
            P(),
        ),
        out_specs=P("table", "dp"),
        check_vma=False,
    )
```

```python
import functools

import jax
import jax.numpy as jnp
from jax import lax
from jax.experimental import pallas as pl
from jax.experimental.pallas import tpu as pltpu
from jax.sharding import PartitionSpec as P

ROWS = 128
TOUCH = 32
OWN = 8
NX = 4
NY = 4
NZ = 8
PARTS = 2
PART = ROWS // PARTS
PAIRED = TOUCH // PARTS
BLOCK = 128
STRIDE = BLOCK + 8
STEPS = PARTS * NZ // 2
SPAN = 4
HALF = SPAN // 2
LAG3 = 2
LAG4 = 3
LAG5 = 7
MESH = pl.DeviceIdType.MESH
BF = jnp.bfloat16
F32 = jnp.float32


def kernel(scale_ref, slots_ref, cells_hbm, codes_hbm, grad_hbm, out_ref,
           cells, codes, grad, row_of, tile_of_pair, weight_of, table, coefs, grads,
           own, pair_out, pair_in, opp_out, opp_in, near_out, near_in, keep, fin0, tiles, got, acc,
           cell_sem, code_sem, grad_sem, pair_send, pair_recv,
           opp_send, opp_recv, near_send, near_recv, tile_send, tile_recv):
    dp = lax.axis_index("dp")
    group = lax.axis_index("table")
    x, c = lax.div(dp, 2), lax.rem(dp, 2)
    y, z = lax.div(group, NZ), lax.rem(group, NZ)
    pairs, tokens = cells.shape
    heads = scale_ref.shape[0]
    per = pairs // heads
    blocks = tokens // BLOCK
    partner = (x * 2 + 1 - c, group)
    ahead = (lax.rem(x + 1, NX) * 2 + c, group)
    behind = (lax.rem(x + NX - 1, NX) * 2 + c, group)
    sides = (ahead, behind)

    def dz_of(s, i):
        far = lax.rem(s, NZ // 2)
        return lax.rem(NZ // 2 + far if i == 0 else NZ // 2 - 1 - far, NZ)

    def z_of(s, i):
        return lax.rem(z + dz_of(s, i), NZ)

    def source_of(s, i, k):
        return k * NZ + lax.rem(z + NZ - dz_of(s, i), NZ)

    def block_start(b):
        return pl.multiple_of(b * BLOCK, BLOCK)

    barrier = pltpu.get_barrier_semaphore()

    def greet(k, carry):
        pl.semaphore_signal(
            barrier, inc=1, device_id=(dp, lax.rem(group + k, NY * NZ)), device_id_type=MESH
        )
        return carry

    def cell_copy(b):
        cut = pl.ds(block_start(b), BLOCK)
        return pltpu.make_async_copy(cells_hbm.at[:, cut], cells.at[:, cut], cell_sem.at[b])

    def code_copy(b):
        cut = pl.ds(block_start(b), BLOCK)
        return pltpu.make_async_copy(codes_hbm.at[:, cut], codes.at[:, cut], code_sem.at[b])

    def grad_copy(b):
        cut = pl.ds(block_start(b), BLOCK)
        return pltpu.make_async_copy(grad_hbm.at[cut, :], grad.at[cut, :], grad_sem.at[b])

    for b in range(blocks):
        cell_copy(b).start()
        code_copy(b).start()
        grad_copy(b).start()
    for peer in (partner, ahead, behind):
        pl.semaphore_signal(barrier, inc=1, device_id=peer, device_id_type=MESH)
    lax.fori_loop(1, NY * NZ, greet, 0)
    acc[...] = jnp.zeros_like(acc)

    def pair_copy(q):
        return pltpu.make_async_remote_copy(
            src_ref=pair_out.at[q], dst_ref=pair_in.at[q],
            send_sem=pair_send.at[q], recv_sem=pair_recv.at[q],
            device_id=partner, device_id_type=MESH,
        )

    def opp_copy(q, side):
        return pltpu.make_async_remote_copy(
            src_ref=opp_out.at[q, side], dst_ref=opp_in.at[q, side],
            send_sem=opp_send.at[q, side], recv_sem=opp_recv.at[q, side],
            device_id=sides[side], device_id_type=MESH,
        )

    def near_copy(q, side, part):
        return pltpu.make_async_remote_copy(
            src_ref=near_out.at[q, side, part], dst_ref=near_in.at[q, side, part],
            send_sem=near_send.at[q, side, part], recv_sem=near_recv.at[q, side, part],
            device_id=sides[side], device_id_type=MESH,
        )

    def tile_copy(s, i, k):
        return pltpu.make_async_remote_copy(
            src_ref=tiles.at[s, i, k], dst_ref=got.at[s, i, y],
            send_sem=tile_send.at[s, i, k], recv_sem=tile_recv.at[s, i, y],
            device_id=(dp, k * NZ + z_of(s, i)), device_id_type=MESH,
        )

    def tile_arrival(s, i, k):
        return pltpu.make_async_remote_copy(
            src_ref=tiles.at[s, i, k], dst_ref=got.at[s, i, k],
            send_sem=tile_send.at[s, i, k], recv_sem=tile_recv.at[s, i, k],
            device_id=(dp, k * NZ + z_of(s, i)), device_id_type=MESH,
        )

    def stays(s, i, k):
        return (dz_of(s, i) == 0) & (y == k)

    def prepare(b):
        cell_copy(b).wait()
        code_copy(b).wait()
        cut = pl.ds(block_start(b), BLOCK)
        cell = cells[:, cut]
        row_of[cut, :] = (cell & (ROWS - 1)).astype(F32).astype(BF).T
        tile_of_pair[cut, :] = (cell >> 7).astype(F32).astype(BF).T
        weight = jnp.concatenate(
            [
                codes[h * per : (h + 1) * per, cut].astype(F32) * (scale_ref[h] / 128.0)
                for h in range(heads)
            ],
            axis=0,
        )
        weight_of[cut, :] = weight.astype(BF).T
        grad_copy(b).wait()
        for k in range(2 * NX):
            core = (1 - c) if k < NX else c
            block = lax.rem(x + k % NX, NX) * 2 + core
            columns = pl.ds(pl.multiple_of(block * ROWS, ROWS), ROWS)
            grads[k * ROWS : (k + 1) * ROWS, cut] = grad[cut, columns].T

    row_iota = lax.broadcasted_iota(jnp.int32, (PART, pairs), 0).astype(F32).astype(BF)
    tile_iota = lax.broadcasted_iota(jnp.int32, (TOUCH, pairs), 0).astype(F32).astype(BF)
    one = jnp.ones((), BF)
    zero = jnp.zeros((), BF)

    def coefficients(t):
        part = lax.div(t, blocks)
        start = block_start(lax.rem(t, blocks))
        shift = (part * PART).astype(F32).astype(BF)
        for v in range(BLOCK // 16):
            sixteen = pl.ds(pl.multiple_of(start + v * 16, 16), 16)
            row = row_of[sixteen, :] - shift
            tile = tile_of_pair[sixteen, :]
            weights = weight_of[sixteen, :]
            for u in range(16):
                row_hot = jnp.where(
                    jnp.broadcast_to(row[u : u + 1, :], (PART, pairs)) == row_iota, one, zero
                ).astype(jnp.float8_e4m3fn)
                tile_hot = jnp.where(
                    jnp.broadcast_to(tile[u : u + 1, :], (TOUCH, pairs)) == tile_iota,
                    jnp.broadcast_to(weights[u : u + 1, :], (TOUCH, pairs)),
                    zero,
                )
                result = lax.dot_general(
                    tile_hot, row_hot, (((1,), (1,)), ((), ())), preferred_element_type=F32
                )
                table[pl.ds(v * 16 + u, PAIRED, stride=STRIDE), :] = jnp.concatenate(
                    [result[k * PAIRED : (k + 1) * PAIRED] for k in range(PARTS)], axis=1
                )
        for j in range(PAIRED):
            coefs[part * PAIRED + j, pl.ds(start, BLOCK), :] = table[
                j * STRIDE : j * STRIDE + BLOCK, :
            ].astype(BF)

    def product(s, which):
        part = lax.div(s, NZ // 2) * PAIRED
        operand = jnp.concatenate(
            [coefs[part + a * NZ + z_of(s, i)] for i in range(2) for a in range(2)], axis=1
        )
        return jnp.dot(
            grads[which * NX * ROWS : (which + 1) * NX * ROWS, :], operand,
            preferred_element_type=F32,
        )

    def stage1(s):
        theirs = product(s, 0).astype(BF)
        for r in range(NX):
            for i in range(SPAN):
                pair_out[s, r, i] = theirs[r * ROWS : (r + 1) * ROWS, i * ROWS : (i + 1) * ROWS]

        @pl.when(s == 0)
        def _():
            pl.semaphore_wait(barrier, NY * NZ + 2)

        pair_copy(s).start()
        mine = product(s, 1)
        slot = lax.rem(s, 2)
        for r in range(NX):
            for i in range(SPAN):
                own[slot, r, i] = mine[r * ROWS : (r + 1) * ROWS, i * ROWS : (i + 1) * ROWS]

    def stage2(q):
        pair_copy(q).wait_recv()
        slot = lax.rem(q, 2)

        def summed(r, half):
            lo = half * HALF
            return own[slot, r, lo : lo + HALF] + pair_in[q, r, lo : lo + HALF].astype(F32)

        for side in range(2):
            opp_out[q, side] = summed(2, side).astype(BF)
            opp_copy(q, side).start()
        for side in range(2):
            r = 1 if side == 0 else NX - 1
            near_out[q, side, 0] = summed(r, 1 - side).astype(BF)
            near_copy(q, side, 0).start()
        for side in range(2):
            r = 1 if side == 0 else NX - 1
            keep[lax.rem(q, 4), side] = summed(r, side)
        for half in range(2):
            fin0[lax.rem(q, 8), half] = summed(0, half)

    def stage3(q):
        slot = lax.rem(q, 4)
        for side in range(2):
            opp_copy(q, side).wait_recv()
            near_out[q, side, 1] = (keep[slot, side] + opp_in[q, side].astype(F32)).astype(BF)
            near_copy(q, side, 1).start()

    def stage4(q):
        eight = lax.rem(q, 8)
        for side in range(2):
            for part in range(2):
                near_copy(q, side, part).wait_recv()
        for i in range(2):
            total = fin0[eight, i]
            for side in range(2):
                total = total + near_in[q, side, 1 if side == i else 0].astype(F32)
            for a in range(HALF):
                turned = total[a].T.astype(BF)
                for k in range(PARTS):
                    tiles[q, i, a + HALF * k] = turned[k * PART : (k + 1) * PART]
            for k in range(NY):
                @pl.when(jnp.logical_not(stays(q, i, k)))
                def _():
                    tile_copy(q, i, k).start()

    def gather(s):
        for i in range(2):
            for k in range(NY):
                @pl.when(jnp.logical_not(stays(s, i, k)))
                def _():
                    tile_arrival(s, i, k).wait_recv()

                @pl.when(stays(s, i, k))
                def _():
                    got[s, i, k] = tiles[s, i, k]

        pieces = [(i, k) for i in range(2) for k in range(NY)]
        slots = [slots_ref[source_of(s, i, k), group] for i, k in pieces]
        parts = [got[s, i, k].astype(F32) for i, k in pieces]
        part = lax.div(s, NZ // 2)
        for o in range(OWN):
            total = acc[o, part]
            for slot, value in zip(slots, parts):
                total = total + jnp.where(slot == o, value, 0.0)
            acc[o, part] = total

    def more(s):
        def one_block(half, carry):
            coefficients(blocks + half)
            return carry

        lax.fori_loop(3 * (s - 1), lax.min(3 * s, blocks), one_block, 0)

    def step(t, carry):
        s = t - blocks
        pl.when(t < blocks)(lambda: prepare(t))
        pl.when((s >= 0) & (s < STEPS))(lambda: stage1(s))
        pl.when(t < blocks)(lambda: coefficients(t))
        pl.when((s >= 1) & (s < STEPS + 1))(lambda: stage2(s - 1))
        pl.when((s >= LAG3) & (s < STEPS + LAG3))(lambda: stage3(s - LAG3))
        pl.when((s >= LAG4) & (s < STEPS + LAG4))(lambda: stage4(s - LAG4))
        pl.when(s >= LAG5)(lambda: gather(s - LAG5))
        pl.when((s >= 1) & (s < 4))(lambda: more(s))
        return carry

    lax.fori_loop(0, blocks + STEPS + LAG5, step, 0)

    for k in range(OWN):
        for h in range(PARTS):
            out_ref[k * ROWS + h * PART : k * ROWS + (h + 1) * PART, :] = acc[k, h].astype(BF)

    def drain(q, carry):
        pair_copy(q).wait_send()
        for side in range(2):
            opp_copy(q, side).wait_send()
            for part in range(2):
                near_copy(q, side, part).wait_send()
        for i in range(2):
            for k in range(NY):
                @pl.when(jnp.logical_not(stays(q, i, k)))
                def _():
                    tile_arrival(q, i, k).wait_send()
        return carry

    lax.fori_loop(0, STEPS, drain, 0)


def body(out_grad, pair_cells, weight_codes, head_scale, touch_slots):
    tokens, width = out_grad.shape
    pairs = pair_cells.shape[1] * pair_cells.shape[2]
    cells = pair_cells.transpose(1, 2, 0).reshape(pairs, tokens)
    codes = weight_codes.transpose(1, 2, 0).reshape(pairs, tokens)
    blocks = tokens // BLOCK
    square = (ROWS, ROWS)
    piece = (PART, ROWS)
    dma = pltpu.SemaphoreType.DMA
    smem = pl.BlockSpec(memory_space=pltpu.SMEM)
    hbm = pl.BlockSpec(memory_space=pltpu.HBM)
    operands = [
        pltpu.with_memory_space_constraint(array, pltpu.HBM)
        for array in (
            head_scale,
            touch_slots.reshape(touch_slots.shape[0], -1),
            cells,
            codes,
            out_grad,
        )
    ]
    return pl.pallas_call(
        kernel,
        in_specs=[smem, smem, hbm, hbm, hbm],
        out_specs=pl.BlockSpec(memory_space=pltpu.VMEM),
        out_shape=jax.ShapeDtypeStruct((OWN * ROWS, ROWS), BF),
        scratch_shapes=[
            pltpu.VMEM((pairs, tokens), jnp.int32),
            pltpu.VMEM((pairs, tokens), jnp.int32),
            pltpu.VMEM((tokens, width), BF),
            pltpu.VMEM((tokens, pairs), BF),
            pltpu.VMEM((tokens, pairs), BF),
            pltpu.VMEM((tokens, pairs), BF),
            pltpu.VMEM((PAIRED * STRIDE, ROWS), F32),
            pltpu.VMEM((PARTS * PAIRED, tokens, ROWS), BF),
            pltpu.VMEM((width, tokens), BF),
            pltpu.VMEM((2, NX, SPAN) + square, F32),
            pltpu.VMEM((STEPS, NX, SPAN) + square, BF),
            pltpu.VMEM((STEPS, NX, SPAN) + square, BF),
            pltpu.VMEM((STEPS, 2, HALF) + square, BF),
            pltpu.VMEM((STEPS, 2, HALF) + square, BF),
            pltpu.VMEM((STEPS, 2, 2, HALF) + square, BF),
            pltpu.VMEM((STEPS, 2, 2, HALF) + square, BF),
            pltpu.VMEM((4, 2, HALF) + square, F32),
            pltpu.VMEM((8, 2, HALF) + square, F32),
            pltpu.VMEM((STEPS, 2, NY) + piece, BF),
            pltpu.VMEM((STEPS, 2, NY) + piece, BF),
            pltpu.VMEM((OWN, PARTS) + piece, F32),
            dma((blocks,)),
            dma((blocks,)),
            dma((blocks,)),
            dma((STEPS,)),
            dma((STEPS,)),
            dma((STEPS, 2)),
            dma((STEPS, 2)),
            dma((STEPS, 2, 2)),
            dma((STEPS, 2, 2)),
            dma((STEPS, 2, NY)),
            dma((STEPS, 2, NY)),
        ],
        compiler_params=pltpu.CompilerParams(
            collective_id=0,
            has_side_effects=True,
            vmem_limit_bytes=45 << 20,
        ),
        name="value_grad",
    )(*operands)


def solution(mesh):
    return jax.shard_map(
        body,
        mesh=mesh,
        in_specs=(
            P(("dp", "table"), None),
            P(("dp", "table"), None, None),
            P(("dp", "table"), None, None),
            P(),
            P(),
        ),
        out_specs=P("table", "dp"),
        check_vma=False,
    )
```
